512 devices in a mesh: depth: 4 (over y_hi, core), blk: 128 (over z, x, y_lo).
Axes of the slice: x: 4, y: 4 (y_hi: 2, y_lo: 2; y = y_hi * 2 + y_lo), z: 16, core: 2. Of those that a mesh axis runs over, the one named last changes fastest.
Arguments:
- jacobian: bfloat16 [1536, 16384], P(('depth', 'blk')), may hold values from -6 to 6
- gain_inverse: bfloat16 [16384, 16384], P('depth', 'blk'), may hold values from -0.00024414062 to 0.00048828125, as said below
- variance: float32 [1536], P(('depth', 'blk')), may hold values from 2 to 12
Outputs:
- omega_diag: float32 [1536], P(('depth', 'blk'))
The draws below stay inside these ranges and needn't reach their ends.
Inputs may be any that keep to these rules, and one draw needn't show every extreme that they name: gain_inverse is symmetric and positive definite.
All inputs are finite; a program needn't handle non-finite values.
Results may differ from the reference program's by a relative error of at most 0.0003.
Values may be sent and summed in bfloat16 or wider, within the bound.
No kernel may reach another device: no remote copies, remote signals or barrier semaphores. Data moves between devices by JAX's collectives and lax.ppermute only.
A program may use at most 128 MiB of HBM per device.

```python
import math
import jax
import jax.numpy as jnp

S = 16384
M = 1536


def draw_gain_inverse(key, part):
    noise_key = jax.random.fold_in(key, 11)
    gains_key = jax.random.fold_in(key, 23)
    gains = jnp.exp(jax.random.uniform(gains_key, (S,), jnp.float32, jnp.log(0.6), jnp.log(1.6)))
    noise = jax.random.normal(noise_key, (S, S), jnp.float32)
    places = jnp.arange(S).astype(jnp.float32)
    distance = jnp.abs(places[:, None] - places[None, :])
    kernel = jnp.exp(-distance / (S / 4.0))
    ident = (distance == 0.0).astype(jnp.float32)
    rough = (noise + noise.T) * (0.4 / jnp.sqrt(2.0 * S))
    matrix = gains[:, None] * gains[None, :] * (ident + kernel + rough) / (2.0 * S)
    return matrix.astype(jnp.bfloat16)


def block_levels(own_key, dims, split, low, top_value):
    factor_of, own = 1.0, jax.random.fold_in(own_key, 6)
    for axis_at, parts in split:
        heights = jnp.exp(jax.random.uniform(jax.random.fold_in(own, axis_at), (parts,), jnp.float32, low / len(split), top_value / len(split)))
        factor_of = factor_of * jnp.repeat(heights, dims[axis_at] // parts).reshape([-1 if axis == axis_at else 1 for axis in range(len(dims))])
    return factor_of


def bell_draw(rng, extent, scale, reach, split=(), kind=jnp.bfloat16):
    drawn = jax.random.normal(rng, extent, jnp.float32) * scale
    if len(split) > 0:
        drawn = block_levels(rng, extent, split, -0.22, 0.18) * drawn
    return jnp.clip(drawn, min=-reach, max=reach).astype(kind)


def setup_inputs(seed: int = 0) -> dict:
    seeds = jax.random.split(jax.random.key(seed), 4)
    jacobian = bell_draw(seeds[0], (M, S), 1.0, 6.0, ((0, 512),))
    gain_inverse = draw_gain_inverse(jax.random.fold_in(seeds[3], 71), 0)
    variance = jnp.clip(jnp.exp(math.log(12.0) - 1.7917595 * jax.random.uniform(seeds[2], (M,), jnp.float32) ** block_levels(seeds[2], (M,), ((0, 512),), -0.2, 0.2)), 2.0, 12.0)
    return {"jacobian": jacobian, "gain_inverse": gain_inverse, "variance": variance}


def reference(jacobian, gain_inverse, variance):
    projected = jnp.dot(jacobian, gain_inverse, preferred_element_type=jnp.float32)
    quadratic = jnp.sum(projected * jacobian.astype(jnp.float32), axis=1)
    return variance - quadratic
```

```python
import functools

import jax
import jax.numpy as jnp
from jax import lax
from jax.experimental import pallas as pl
from jax.experimental.pallas import tpu as pltpu
from jax.sharding import Mesh
from jax.sharding import PartitionSpec as P

Z = "z"
PLANE = ("yh", "x", "yl")
ALL = ("yh", "core", "z", "x", "yl")
F32 = jnp.float32
BF16 = jnp.bfloat16
TILES = 16
LANES = 128
VMEM = pl.BlockSpec(memory_space=pltpu.VMEM)


def plane_index():
    return (lax.axis_index("yh") * lax.axis_size("x") + lax.axis_index("x")) * lax.axis_size(
        "yl"
    ) + lax.axis_index("yl")


def half_of(c, z):
    t = lax.rem(z - c + TILES, TILES)
    low = jnp.logical_or(t < TILES // 2, jnp.logical_and(t == TILES // 2, c < z))
    return jnp.where(low, 0, 1)


def exchange(parts, axis):
    return lax.all_to_all(parts, axis, split_axis=0, concat_axis=0, tiled=True)


def spread_kernel(rows, chunks, for_columns, in_ref, out_ref, wide):
    c = plane_index()
    z = lax.axis_index(Z)
    half = TILES // 2
    step = rows * chunks
    wide[...] = in_ref[...].astype(F32)
    mine = c if for_columns else z
    top = mine // half
    pieces = []
    for side in range(2):
        chunk_rows = []
        for q in range(chunks):
            base = side * half * step + q
            if for_columns:
                got = jnp.concatenate(
                    [
                        wide[pl.ds(base + r * chunks, half, stride=step), :]
                        for r in range(rows)
                    ],
                    axis=0,
                )
            else:
                got = wide[pl.ds(base, half * rows, stride=chunks), :]
            chunk_rows.append(got.astype(BF16))
        pieces.append(chunk_rows)
    for to in range(TILES):
        if for_columns:
            wanted = jnp.where(to == z, 1, half_of(to, z))
        else:
            wanted = half_of(c, to)
        first = (wanted + top) % 2 == 0

        @pl.when(first)
        def _():
            for q in range(chunks):
                out_ref[to, q] = pieces[0][q]

        @pl.when(jnp.logical_not(first))
        def _():
            for q in range(chunks):
                out_ref[to, q] = pieces[1][q]


def spread(parts, rows, chunks, for_columns):
    return pl.pallas_call(
        functools.partial(spread_kernel, rows, chunks, for_columns),
        out_shape=jax.ShapeDtypeStruct((TILES, chunks, TILES // 2 * rows, LANES), BF16),
        in_specs=[VMEM],
        out_specs=VMEM,
        scratch_shapes=[pltpu.VMEM((TILES * rows * chunks, LANES), F32)],
        cost_estimate=pl.CostEstimate(flops=2_000_000, bytes_accessed=900_000, transcendentals=0),
        name="spread_columns" if for_columns else "spread_rows",
    )(parts)


def tile_kernel(rows, chunks, x_ref, y_ref, own_ref, other_ref, out_ref, wide, left):
    c = plane_index()
    z = lax.axis_index(Z)
    core = lax.axis_index("core")
    half = TILES // 2
    group = half * rows
    total = TILES * group
    deep = chunks // 2 * LANES
    diagonal = c == z
    half_x = half_of(c, z)
    half_y = jnp.where(diagonal, 1, half_x)
    for j in range(chunks):
        for s in range(TILES):
            wide[j, s * group : (s + 1) * group, :] = y_ref[s, j].astype(F32)
    for q in range(chunks):
        side, lane = q // (chunks // 2), q % (chunks // 2) * LANES
        for s in range(TILES):
            left[side, s * group : (s + 1) * group, lane : lane + LANES] = x_ref[s, q]
            column_top = (half_y + s // half) % 2
            first = column_top * (half * group) + s % half
            got = wide[q, pl.ds(first, group, stride=half), :]
            left[side, total + s * group : total + (s + 1) * group, lane : lane + LANES] = got.astype(
                BF16
            )
    acc = jnp.zeros((2 * total, LANES), F32)
    for pair in range(chunks // 2):
        own = jnp.concatenate([own_ref[2 * pair], own_ref[2 * pair + 1]], axis=1)
        other = jnp.concatenate([other_ref[2 * pair], other_ref[2 * pair + 1]], axis=1)
        product = jnp.dot(left[core], own, preferred_element_type=F32)
        product += jnp.dot(left[1 - core], other, preferred_element_type=F32)
        side, lane = pair * 2 // (chunks // 2), pair * 2 % (chunks // 2) * LANES
        rows_x = left[side, :total, lane : lane + 2 * LANES].astype(F32)
        rows_y = left[side, total:, lane : lane + 2 * LANES].astype(F32)
        right = jnp.concatenate([jnp.where(diagonal, rows_x, rows_y), rows_y], axis=0)
        weighted = product * right
        acc += weighted[:, :LANES] + weighted[:, LANES:]
    ones = jnp.ones((8, LANES), F32)
    scale_x = jnp.where(diagonal, 1.0, 2.0)
    for s in range(TILES):
        sums = []
        for start in (s * group, total + s * group):
            sums.append(
                lax.dot_general(
                    ones,
                    acc[start : start + group],
                    (((1,), (1,)), ((), ())),
                    precision=lax.Precision.HIGHEST,
                    preferred_element_type=F32,
                )[:1]
            )
        from_x = sums[0] * scale_x
        from_y = jnp.where(diagonal, sums[1], 0.0)
        low = (half_x + s // half) % 2 == 0
        out_ref[s] = jnp.concatenate(
            [jnp.where(low, from_x, from_y), jnp.where(low, from_y, from_x)], axis=0
        )


def tile(x_rows, y_rows, own, other, rows, chunks):
    group = TILES // 2 * rows
    flops = 2 * 2 * TILES * group * (chunks * LANES) ** 2
    return pl.pallas_call(
        functools.partial(tile_kernel, rows, chunks),
        out_shape=jax.ShapeDtypeStruct((TILES, 2, group), F32),
        in_specs=[VMEM] * 4,
        out_specs=VMEM,
        scratch_shapes=[
            pltpu.VMEM((chunks, TILES * group, LANES), F32),
            pltpu.VMEM((2, 2 * TILES * group, chunks // 2 * LANES), BF16),
        ],
        cost_estimate=pl.CostEstimate(flops=flops, bytes_accessed=4_000_000, transcendentals=0),
        compiler_params=pltpu.CompilerParams(vmem_limit_bytes=48 * 1024 * 1024),
        name="tile",
    )(x_rows, y_rows, own, other)


def retile(gain):
    core = lax.axis_index("core")
    panel = gain.shape[1]
    halves = gain.reshape(TILES // 4, 2, -1, panel)
    kept = lax.dynamic_index_in_dim(halves, core, 1, keepdims=False)
    given = lax.dynamic_index_in_dim(halves, 1 - core, 1, keepdims=False)
    swap = [(0, 1), (1, 0)]
    taken = lax.ppermute(given, "core", swap)
    first = jnp.where(core == 0, kept, taken)
    second = jnp.where(core == 0, taken, kept)
    own = exchange(jnp.concatenate([first, second], axis=0), ("x", "yl"))
    return own, lax.ppermute(own, "core", swap)


def shards(jacobian, gain, variance):
    rows, width = jacobian.shape
    chunks = width // TILES // LANES
    parts = jacobian.reshape(rows, TILES, chunks, LANES).transpose(1, 0, 2, 3)
    parts = parts.reshape(TILES * rows * chunks, LANES)
    by_rows = exchange(parts, PLANE)
    by_columns = exchange(parts, Z)
    x_rows = exchange(spread(by_rows, rows, chunks, False), Z)
    y_rows = exchange(spread(by_columns, rows, chunks, True), PLANE)
    own, other = retile(gain)
    partial = tile(x_rows, y_rows, own, other, rows, chunks)
    along_z = exchange(partial, Z).sum(axis=0)
    in_plane = exchange(along_z.reshape(TILES, rows), PLANE).sum(axis=0)
    return variance - in_plane


def solution(mesh):
    devices = mesh.devices.reshape(2, 2, TILES, 4, 2)
    return jax.shard_map(
        shards,
        mesh=Mesh(devices, ALL),
        in_specs=(P(ALL, None), P(("yh", "core"), ("z", "x", "yl")), P(ALL)),
        out_specs=P(ALL),
        check_vma=False,
    )
```

```python
import functools

import jax
import jax.numpy as jnp
from jax import lax
from jax.experimental import pallas as pl
from jax.experimental.pallas import tpu as pltpu
from jax.sharding import Mesh
from jax.sharding import PartitionSpec as P

PLANE = ("yh", "x", "yl")
ALL = ("yh", "core", "z", "x", "yl")
F32 = jnp.float32
BF16 = jnp.bfloat16
TILES = 16
HALF = TILES // 2
LANES = 128
VMEM = pl.BlockSpec(memory_space=pltpu.VMEM)


def plane_index():
    return (lax.axis_index("yh") * 4 + lax.axis_index("x")) * 2 + lax.axis_index("yl")


def half_of(c, z):
    t = lax.rem(z - c + TILES, TILES)
    high = jnp.where(z >= HALF, 1, 0)
    return jnp.where(t == 0, high, jnp.where(t == HALF, 1 - high, jnp.where(t < HALF, 0, 1)))


def slot_of(c, z):
    t = lax.rem(z - c + TILES, TILES)
    high = jnp.where(z >= HALF, 1, 0)
    slot = jnp.where(half_of(c, z) == 0, t - high, TILES - t - (1 - high))
    return jnp.where(t == 0, HALF, slot)


def exchange(parts, axis):
    return lax.all_to_all(parts, axis, split_axis=0, concat_axis=0, tiled=True)


def pick_kernel(in_ref, out_ref):
    half = lax.rem(lax.axis_index("yh") + lax.axis_index("z") // HALF, 2)
    for z in range(TILES):
        high = 1 if z >= HALF else 0
        for slot in range(HALF):
            first = (z - slot - high) % TILES
            second = (z + slot + 1 - high) % TILES
            out_ref[z, slot] = in_ref[jnp.where(half == 0, first, second)]
        out_ref[z, HALF] = in_ref[z]


def pick(parts):
    return pl.pallas_call(
        pick_kernel,
        out_shape=jax.ShapeDtypeStruct((TILES, HALF + 1, *parts.shape[1:]), BF16),
        in_specs=[VMEM],
        out_specs=VMEM,
        cost_estimate=pl.CostEstimate(flops=1_000_000, bytes_accessed=900_000, transcendentals=0),
        compiler_params=pltpu.CompilerParams(vmem_limit_bytes=4 * 1024 * 1024),
        name="pick",
    )(parts)


def spread_kernel(rows, chunks, in_ref, out_ref, wide):
    z = lax.axis_index("z")
    top = lax.axis_index("yh")
    block = rows * chunks
    step = (HALF + 1) * block
    for s in range(TILES):
        wide[s * step : (s + 1) * step, :] = in_ref[s].astype(F32)

    @pl.loop(0, TILES)
    def _(to):
        half_x = half_of(to, z)
        half_y = jnp.where(to == z, 1 - half_x, half_x)
        base_x = lax.rem(half_x + top, 2) * (HALF * step) + slot_of(to, z) * block
        base_y = lax.rem(half_y + top, 2) * (HALF * step) + HALF * block
        for side, base in ((0, base_x), (1, base_y)):
            for q in range(chunks):
                got = [
                    wide[pl.ds(base + r * chunks + q, HALF, stride=step), :] for r in range(rows)
                ]
                out_ref[to, side * chunks + q] = jnp.concatenate(got, axis=0).astype(BF16)


def spread(parts, rows, chunks):
    return pl.pallas_call(
        functools.partial(spread_kernel, rows, chunks),
        out_shape=jax.ShapeDtypeStruct((TILES, 2 * chunks, HALF * rows, LANES), BF16),
        in_specs=[VMEM],
        out_specs=VMEM,
        scratch_shapes=[pltpu.VMEM((TILES * parts.shape[1], LANES), F32)],
        cost_estimate=pl.CostEstimate(flops=4_000_000, bytes_accessed=2_500_000, transcendentals=0),
        compiler_params=pltpu.CompilerParams(vmem_limit_bytes=8 * 1024 * 1024),
        name="spread",
    )(parts)


def tile_kernel(rows, chunks, xy_ref, own_ref, other_ref, out_ref, narrow, left):
    z = lax.axis_index("z")
    x = lax.axis_index("x")
    yl = lax.axis_index("yl")
    core = lax.axis_index("core")
    c = plane_index()
    group = HALF * rows
    total = TILES * group
    near = chunks // 2
    diagonal = c == z
    half_x = half_of(c, z)
    for q in range(chunks):
        side, lane = q // near, q % near * LANES
        for s in range(TILES):
            for kind in range(2):
                start = kind * total + s * group
                got = xy_ref[s, kind * chunks + q]
                left[side, start : start + group, lane : lane + LANES] = got
                narrow[kind, q, s * group : (s + 1) * group, :] = got
    acc_x = jnp.zeros((total, LANES), F32)
    acc_y = jnp.zeros((total, LANES), F32)
    kind_x = jnp.where(diagonal, 0, 1)
    for m in range(chunks // 2):
        own = jnp.concatenate([own_ref[2 * m], own_ref[2 * m + 1]], axis=1)
        other = jnp.concatenate([other_ref[2 * m], other_ref[2 * m + 1]], axis=1)
        product = jnp.dot(left[core], own, preferred_element_type=F32)
        product += jnp.dot(left[1 - core], other, preferred_element_type=F32)
        for n in range(2):
            k = (x ^ m) * 2 + (yl ^ n)
            part = product[:, n * LANES : (n + 1) * LANES]
            acc_x += part[:total] * narrow[kind_x, k].astype(F32)
            acc_y += part[total:] * narrow[1, k].astype(F32)
    ones = jnp.ones((8, LANES), F32)
    scale_x = jnp.where(diagonal, 1.0, 2.0)
    for s in range(TILES):
        from_x, from_y = (
            lax.dot_general(
                ones,
                acc[s * group : (s + 1) * group],
                (((1,), (1,)), ((), ())),
                precision=lax.Precision.HIGHEST,
                preferred_element_type=F32,
            )[:1]
            for acc in (acc_x, acc_y)
        )
        from_x = from_x * scale_x
        from_y = jnp.where(diagonal, from_y, 0.0)
        low = lax.rem(half_x + s // HALF, 2) == 0
        out_ref[s] = jnp.concatenate(
            [jnp.where(low, from_x, from_y), jnp.where(low, from_y, from_x)], axis=0
        )


def tile(xy, own, other, rows, chunks):
    total = TILES * HALF * rows
    flops = 2 * 2 * total * (chunks * LANES) ** 2
    return pl.pallas_call(
        functools.partial(tile_kernel, rows, chunks),
        out_shape=jax.ShapeDtypeStruct((TILES, 2, HALF * rows), F32),
        in_specs=[VMEM] * 3,
        out_specs=VMEM,
        scratch_shapes=[
            pltpu.VMEM((2, chunks, total, LANES), BF16),
            pltpu.VMEM((2, 2 * total, chunks // 2 * LANES), BF16),
        ],
        cost_estimate=pl.CostEstimate(flops=flops, bytes_accessed=4_000_000, transcendentals=0),
        compiler_params=pltpu.CompilerParams(vmem_limit_bytes=16 * 1024 * 1024),
        name="tile",
    )(xy, own, other)


def retile(gain):
    core, x, yl = (lax.axis_index(name) for name in ("core", "x", "yl"))
    panel = gain.shape[1]
    halves = gain.reshape(TILES // 4, 2, -1, panel)
    kept = lax.dynamic_index_in_dim(halves, core, 1, keepdims=False)
    given = lax.dynamic_index_in_dim(halves, 1 - core, 1, keepdims=False)
    swap = [(0, 1), (1, 0)]
    taken = lax.ppermute(given, "core", swap)
    first = jnp.where(core == 0, kept, taken)
    second = jnp.where(core == 0, taken, kept)
    blocks = jnp.concatenate([first, second], axis=0)
    got = []
    for m in range(4):
        for n in range(2):
            block = lax.dynamic_index_in_dim(blocks, (x ^ m) * 2 + (yl ^ n), 0, keepdims=False)
            if m or n:
                turn = [
                    (a * 2 + b, (a ^ m) * 2 + (b ^ n)) for a in range(4) for b in range(2)
                ]
                block = lax.ppermute(block, ("x", "yl"), turn)
            got.append(block)
    own = jnp.stack(got)
    return own, lax.ppermute(own, "core", swap)


def shards(jacobian, gain, variance):
    rows, width = jacobian.shape
    chunks = width // TILES // LANES
    parts = jacobian.reshape(rows, TILES, chunks, LANES).transpose(1, 0, 2, 3)
    parts = parts.reshape(TILES, rows * chunks, LANES)
    planes = exchange(pick(parts), "z")
    planes = planes.reshape(TILES, (HALF + 1) * rows * chunks, LANES)
    xy = exchange(spread(planes, rows, chunks), PLANE)
    own, other = retile(gain)
    partial = tile(xy, own, other, rows, chunks)
    in_plane = exchange(partial, PLANE).sum(axis=0)
    in_plane = in_plane.reshape(2, rows, HALF).transpose(0, 2, 1).reshape(TILES, rows)
    return variance - exchange(in_plane, "z").sum(axis=0)


def solution(mesh):
    devices = mesh.devices.reshape(2, 2, TILES, 4, 2)
    return jax.shard_map(
        shards,
        mesh=Mesh(devices, ALL),
        in_specs=(P(ALL, None), P(("yh", "core"), ("z", "x", "yl")), P(ALL)),
        out_specs=P(ALL),
        check_vma=False,
    )
```

```python
import functools

import jax
import jax.numpy as jnp
from jax import lax
from jax.experimental import pallas as pl
from jax.experimental.pallas import tpu as pltpu
from jax.sharding import Mesh
from jax.sharding import PartitionSpec as P


PLANE = ("yh", "x", "yl")
ALL = ("yh", "core", "z", "x", "yl")
F32 = jnp.float32
BF16 = jnp.bfloat16
TILES = 16
HALF = TILES // 2
LANES = 128
VMEM = pl.BlockSpec(memory_space=pltpu.VMEM)


def plane_index():
    return (lax.axis_index("yh") * 4 + lax.axis_index("x")) * 2 + lax.axis_index("yl")


def half_of(c, z):
    t = lax.rem(z - c + TILES, TILES)
    high = jnp.where(z >= HALF, 1, 0)
    return jnp.where(t == 0, high, jnp.where(t == HALF, 1 - high, jnp.where(t < HALF, 0, 1)))


def slot_of(c, z):
    t = lax.rem(z - c + TILES, TILES)
    high = jnp.where(z >= HALF, 1, 0)
    slot = jnp.where(half_of(c, z) == 0, t - high, TILES - t - (1 - high))
    return jnp.where(t == 0, HALF, slot)


def exchange(parts, axis):
    return lax.all_to_all(parts, axis, split_axis=0, concat_axis=0, tiled=True)


def pick_kernel(in_ref, out_ref):
    half = lax.rem(lax.axis_index("yh") + lax.axis_index("z") // HALF, 2)
    for z in range(TILES):
        high = 1 if z >= HALF else 0
        for slot in range(HALF):
            first = (z - slot - high) % TILES
            second = (z + slot + 1 - high) % TILES
            out_ref[z, slot] = in_ref[jnp.where(half == 0, first, second)]
        out_ref[z, HALF] = in_ref[z]


def pick(parts):
    return pl.pallas_call(
        pick_kernel,
        out_shape=jax.ShapeDtypeStruct((TILES, HALF + 1, *parts.shape[1:]), BF16),
        in_specs=[VMEM],
        out_specs=VMEM,
        cost_estimate=pl.CostEstimate(flops=1_000_000, bytes_accessed=900_000, transcendentals=0),
        compiler_params=pltpu.CompilerParams(vmem_limit_bytes=4 * 1024 * 1024),
        name="pick",
    )(parts)


def spread_kernel(rows, chunks, in_ref, out_ref, wide):
    z = lax.axis_index("z")
    top = lax.axis_index("yh")
    block = rows * chunks
    step = (HALF + 1) * block
    for s in range(TILES):
        wide[s * step : (s + 1) * step, :] = in_ref[s].astype(F32)

    @pl.loop(0, TILES)
    def _(to):
        half_x = half_of(to, z)
        half_y = jnp.where(to == z, 1 - half_x, half_x)
        base_x = lax.rem(half_x + top, 2) * (HALF * step) + slot_of(to, z) * block
        base_y = lax.rem(half_y + top, 2) * (HALF * step) + HALF * block
        for side, base in ((0, base_x), (1, base_y)):
            for q in range(chunks):
                got = [
                    wide[pl.ds(base + r * chunks + q, HALF, stride=step), :] for r in range(rows)
                ]
                out_ref[to, side * chunks + q] = jnp.concatenate(got, axis=0).astype(BF16)


def spread(parts, rows, chunks):
    return pl.pallas_call(
        functools.partial(spread_kernel, rows, chunks),
        out_shape=jax.ShapeDtypeStruct((TILES, 2 * chunks, HALF * rows, LANES), BF16),
        in_specs=[VMEM],
        out_specs=VMEM,
        scratch_shapes=[pltpu.VMEM((TILES * parts.shape[1], LANES), F32)],
        cost_estimate=pl.CostEstimate(flops=4_000_000, bytes_accessed=2_500_000, transcendentals=0),
        compiler_params=pltpu.CompilerParams(vmem_limit_bytes=8 * 1024 * 1024),
        name="spread",
    )(parts)


def tile_kernel(rows, chunks, xy_ref, *refs):
    *column_refs, out_ref, narrow, left = refs
    z = lax.axis_index("z")
    x = lax.axis_index("x")
    yl = lax.axis_index("yl")
    c = plane_index()
    group = HALF * rows
    total = TILES * group
    diagonal = c == z
    half_x = half_of(c, z)
    for q in range(chunks):
        lane = q * LANES
        for s in range(TILES):
            for kind in range(2):
                start = kind * total + s * group
                got = xy_ref[s, kind * chunks + q]
                left[start : start + group, lane : lane + LANES] = got
                narrow[kind, q, s * group : (s + 1) * group, :] = got
    acc_x = jnp.zeros((total, LANES), F32)
    acc_y = jnp.zeros((total, LANES), F32)
    kind_x = jnp.where(diagonal, 0, 1)
    for m in range(chunks // 2):
        columns = jnp.concatenate([column_refs[2 * m][...], column_refs[2 * m + 1][...]], axis=1)
        product = jnp.dot(left[...], columns, preferred_element_type=F32)
        for n in range(2):
            k = (x ^ m) * 2 + (yl ^ n)
            part = product[:, n * LANES : (n + 1) * LANES]
            acc_x += part[:total] * narrow[kind_x, k].astype(F32)
            acc_y += part[total:] * narrow[1, k].astype(F32)
    ones = jnp.ones((8, LANES), F32)
    scale_x = jnp.where(diagonal, 1.0, 2.0)
    for s in range(TILES):
        from_x, from_y = (
            lax.dot_general(
                ones,
                acc[s * group : (s + 1) * group],
                (((1,), (1,)), ((), ())),
                precision=lax.Precision.HIGHEST,
                preferred_element_type=F32,
            )[:1]
            for acc in (acc_x, acc_y)
        )
        from_x = from_x * scale_x
        from_y = jnp.where(diagonal, from_y, 0.0)
        low = lax.rem(half_x + s // HALF, 2) == 0
        out_ref[s] = jnp.concatenate(
            [jnp.where(low, from_x, from_y), jnp.where(low, from_y, from_x)], axis=0
        )


def tile(xy, columns, rows, chunks):
    total = TILES * HALF * rows
    flops = 2 * 2 * total * (chunks * LANES) ** 2
    return pl.pallas_call(
        functools.partial(tile_kernel, rows, chunks),
        out_shape=jax.ShapeDtypeStruct((TILES, 2, HALF * rows), F32),
        in_specs=[VMEM] * (1 + len(columns)),
        out_specs=VMEM,
        scratch_shapes=[
            pltpu.VMEM((2, chunks, total, LANES), BF16),
            pltpu.VMEM((2 * total, chunks * LANES), BF16),
        ],
        cost_estimate=pl.CostEstimate(flops=flops, bytes_accessed=4_000_000, transcendentals=0),
        compiler_params=pltpu.CompilerParams(vmem_limit_bytes=16 * 1024 * 1024),
        name="tile",
    )(xy, *columns)


def retile(gain):
    core, x, yl = (lax.axis_index(name) for name in ("core", "x", "yl"))
    taken = lax.ppermute(gain, "core", [(0, 1), (1, 0)])
    own, taken = (part.reshape(TILES // 4, -1, gain.shape[1]) for part in (gain, taken))
    got = []
    for m in range(4):
        for n in range(2):
            to_x, to_y = x ^ m, yl ^ n
            at = (to_x % 2) * 2 + to_y
            kept, given = (lax.dynamic_index_in_dim(part, at, 0, keepdims=False) for part in (own, taken))
            block = jnp.where(to_x // 2 == core, kept, given)
            if m or n:
                turn = [(a * 2 + b, (a ^ m) * 2 + (b ^ n)) for a in range(4) for b in range(2)]
                block = lax.ppermute(block, ("x", "yl"), turn)
            got.append(block)
    return got


def shards(jacobian, gain, variance):
    rows, width = jacobian.shape
    chunks = width // TILES // LANES
    parts = jacobian.reshape(rows, TILES, chunks, LANES).transpose(1, 0, 2, 3)
    parts = parts.reshape(TILES, rows * chunks, LANES)
    planes = exchange(pick(parts), "z")
    columns = retile(gain)
    planes = planes.reshape(TILES, (HALF + 1) * rows * chunks, LANES)
    sent = spread(planes, rows, chunks)
    xy = exchange(sent, PLANE)
    partial = tile(xy, columns, rows, chunks)
    in_plane = exchange(partial, PLANE).sum(axis=0)
    in_plane = in_plane.reshape(2, rows, HALF).transpose(0, 2, 1).reshape(TILES, rows)
    return variance - exchange(in_plane, "z").sum(axis=0)


def solution(mesh):
    devices = mesh.devices.reshape(2, 2, TILES, 4, 2)
    return jax.shard_map(
        shards,
        mesh=Mesh(devices, ALL),
        in_specs=(P(ALL, None), P(("yh", "core"), ("z", "x", "yl")), P(ALL)),
        out_specs=P(ALL),
        check_vma=False,
    )
```

```python
import functools
import itertools

import jax
import jax.numpy as jnp
from jax import lax
from jax.experimental import pallas as pl
from jax.experimental.pallas import tpu as pltpu
from jax.sharding import Mesh
from jax.sharding import PartitionSpec as P


PLANE = ("yh", "x", "yl")
ALL = ("yh", "core", "z", "x", "yl")
F32 = jnp.float32
BF16 = jnp.bfloat16
TILES = 16
HALF = TILES // 2
QUAD = 4
FAR = 7
NEAR = 8
LANES = 128
VMEM = pl.BlockSpec(memory_space=pltpu.VMEM)


def plane_index():
    return (lax.axis_index("yh") * 4 + lax.axis_index("x")) * 2 + lax.axis_index("yl")


def half_of(c, z):
    apart = jnp.where(c // QUAD < z // QUAD, 1, 0) ^ (c & 1) ^ (z & 1)
    turn = (z - c) & 3
    beside = jnp.where(turn == 2, 1 ^ ((z >> 1) & 1), turn >> 1)
    return jnp.where(c // QUAD == z // QUAD, beside, apart)


def block_for(z, half, quad, second):
    beside = z ^ 2 if second else (z // QUAD) * QUAD + ((z + 2 * half - 1) & 3)
    apart = QUAD * quad + 2 * second + (half ^ jnp.where(quad < z // QUAD, 1, 0) ^ (z & 1))
    return jnp.where(quad == z // QUAD, beside, apart)


def exchange(parts, axis):
    return lax.all_to_all(parts, axis, split_axis=0, concat_axis=0, tiled=True)


def pick_kernel(in_ref, far_ref, near_ref):
    mine = lax.axis_index("z")
    half = lax.axis_index("yh") ^ (mine & 1)
    for z in range(TILES):
        for slot in range(FAR - 1):
            quad = slot // 2 + jnp.where(slot // 2 >= mine // QUAD, 1, 0)
            far_ref[z, slot] = in_ref[block_for(z, half, quad, slot % 2)]
        far_ref[z, FAR - 1] = in_ref[z]
    for m in range(QUAD):
        z = mine ^ m
        for slot in range(NEAR):
            quad = slot // 2 + jnp.where(slot // 2 >= mine // QUAD, 1, 0)
            if slot < FAR - 1:
                near_ref[m, slot] = in_ref[block_for(z, 1 - half, quad, slot % 2)]
            else:
                near_ref[m, slot] = in_ref[block_for(z, half, mine // QUAD, slot % 2)]


def pick(parts):
    return pl.pallas_call(
        pick_kernel,
        out_shape=(
            jax.ShapeDtypeStruct((TILES, FAR, *parts.shape[1:]), BF16),
            jax.ShapeDtypeStruct((QUAD, NEAR, *parts.shape[1:]), BF16),
        ),
        in_specs=[VMEM],
        out_specs=(VMEM, VMEM),
        cost_estimate=pl.CostEstimate(flops=1_000_000, bytes_accessed=900_000, transcendentals=0),
        compiler_params=pltpu.CompilerParams(vmem_limit_bytes=4 * 1024 * 1024),
        name="pick",
    )(parts)


def spread_kernel(rows, chunks, far_ref, *refs):
    *near_refs, out_ref, wide, stage = refs
    z = lax.axis_index("z")
    top = lax.axis_index("yh")
    block = rows * chunks
    step = FAR * block
    near_at = TILES * step
    for s in range(TILES):
        wide[s * step : (s + 1) * step, :] = far_ref[s].astype(F32)
    for m in range(QUAD):
        at = near_at + m * NEAR * block
        wide[at : at + NEAR * block, :] = near_refs[m][...].astype(F32)

    @pl.loop(0, TILES)
    def _(to):
        diagonal = to == z
        quad = to // QUAD
        beside = quad == z // QUAD
        half_x = jnp.where(diagonal, 0, half_of(to, z))
        half_y = jnp.where(diagonal, 1, half_x)
        second = jnp.where(beside, jnp.where(((z - to) & 3) == 2, 1, 0), (to >> 1) & 1)
        for k in range(HALF):
            swapped = quad == k // 2
            for side, half in ((0, half_x), (1, half_y)):
                parity = half ^ top
                s = 2 * k + parity
                near_s = (z // QUAD) * QUAD + 2 * (k % 2) + jnp.where(beside, parity, 1 - parity)
                last = FAR - 1
                if side == 0:
                    slot = 2 * (quad - jnp.where(quad > k // 2, 1, 0)) + second
                    far = s * FAR + jnp.where(diagonal, last, slot)
                    near_slot = 2 * (quad - jnp.where(quad > z // QUAD, 1, 0)) + second
                    near_slot = jnp.where(beside, last + second, near_slot)
                    near = TILES * FAR + (near_s ^ z) * NEAR + near_slot
                    use_near = jnp.logical_and(swapped, jnp.logical_not(diagonal))
                else:
                    far = s * FAR + last
                    near = near_s * FAR + last
                    use_near = jnp.logical_and(swapped, jnp.logical_not(beside))
                at = pl.multiple_of(jnp.where(use_near, near, far) * block, HALF)
                stage[side, k * block : (k + 1) * block, :] = wide[pl.ds(at, block), :]
        for side in range(2):
            for q in range(chunks):
                got = [
                    stage[side, pl.ds(r * chunks + q, HALF, stride=block), :] for r in range(rows)
                ]
                out_ref[to, side * chunks + q] = jnp.concatenate(got, axis=0).astype(BF16)


def spread(far, near, rows, chunks):
    block = rows * chunks
    return pl.pallas_call(
        functools.partial(spread_kernel, rows, chunks),
        out_shape=jax.ShapeDtypeStruct((TILES, 2 * chunks, HALF * rows, LANES), BF16),
        in_specs=[VMEM] * (1 + len(near)),
        out_specs=VMEM,
        scratch_shapes=[
            pltpu.VMEM(((TILES * FAR + QUAD * NEAR) * block, LANES), F32),
            pltpu.VMEM((2, HALF * block, LANES), F32),
        ],
        cost_estimate=pl.CostEstimate(flops=4_000_000, bytes_accessed=2_500_000, transcendentals=0),
        compiler_params=pltpu.CompilerParams(vmem_limit_bytes=8 * 1024 * 1024),
        name="spread",
    )(far, *near)


def tile_kernel(rows, chunks, xy_ref, *refs):
    *column_refs, out_ref, narrow, left = refs
    z = lax.axis_index("z")
    x = lax.axis_index("x")
    yl = lax.axis_index("yl")
    core = lax.axis_index("core")
    c = plane_index()
    group = HALF * rows
    total = TILES * group
    diagonal = c == z
    half_x = jnp.where(diagonal, 0, half_of(c, z))
    half_y = jnp.where(diagonal, 1, half_x)
    beside = c // QUAD == z // QUAD
    for q in range(chunks):
        lane = q * LANES
        for s in range(TILES):
            for kind in range(2):
                start = kind * total + s * group
                got = xy_ref[s, kind * chunks + q]
                left[start : start + group, lane : lane + LANES] = got
                narrow[kind, q, s * group : (s + 1) * group, :] = got
    acc_x = jnp.zeros((total, LANES), F32)
    acc_y = jnp.zeros((total, LANES), F32)
    kind_x = jnp.where(diagonal, 0, 1)
    for m in range(chunks // 2):
        columns = jnp.concatenate([column_refs[2 * m][...], column_refs[2 * m + 1][...]], axis=1)
        product = jnp.dot(left[...], columns, preferred_element_type=F32)
        for n in range(2):
            k = ((core ^ (m // 2)) * 2 + ((x & 1) ^ (m % 2))) * 2 + (yl ^ n)
            part = product[:, n * LANES : (n + 1) * LANES]
            acc_x += part[:total] * narrow[kind_x, k].astype(F32)
            acc_y += part[total:] * narrow[1, k].astype(F32)
    ones = jnp.ones((LANES, LANES), F32)
    sum_x, sum_y = (
        jnp.dot(acc, ones, precision=lax.Precision.HIGHEST, preferred_element_type=F32)
        for acc in (acc_x, acc_y)
    )
    lane = lax.broadcasted_iota(jnp.int32, (group, LANES), 1)
    row = lax.broadcasted_iota(jnp.int32, (group, LANES), 0)
    r, k = row // HALF, row % HALF
    scale_x = jnp.where(diagonal, 1.0, 2.0)
    for top in range(2):
        parity = half_x ^ top
        swapped = jnp.logical_and(k // 2 == c // QUAD, jnp.logical_not(beside))
        plane = jnp.where(swapped, (z // QUAD) * QUAD + 2 * (k % 2) + 1 - parity, 2 * k + parity)
        mine_x = lane == r * TILES + plane
        mine_y = jnp.logical_and(lane == r * TILES + 2 * k + (half_y ^ top), diagonal)
        for s in range(top * HALF, (top + 1) * HALF):
            got = jnp.where(mine_x, sum_x[s * group : (s + 1) * group] * scale_x, 0.0)
            got = jnp.where(mine_y, sum_y[s * group : (s + 1) * group], got)
            out_ref[s : s + 1, :] = jnp.sum(got, axis=0, keepdims=True)


def tile(xy, columns, rows, chunks):
    total = TILES * HALF * rows
    flops = 2 * 2 * total * (chunks * LANES) ** 2
    return pl.pallas_call(
        functools.partial(tile_kernel, rows, chunks),
        out_shape=jax.ShapeDtypeStruct((TILES, LANES), F32),
        in_specs=[VMEM] * (1 + len(columns)),
        out_specs=VMEM,
        scratch_shapes=[
            pltpu.VMEM((2, chunks, total, LANES), BF16),
            pltpu.VMEM((2 * total, chunks * LANES), BF16),
        ],
        cost_estimate=pl.CostEstimate(flops=flops, bytes_accessed=4_000_000, transcendentals=0),
        compiler_params=pltpu.CompilerParams(vmem_limit_bytes=16 * 1024 * 1024),
        name="tile",
    )(xy, *columns)


def retile(gain):
    low, yl = lax.axis_index("x") % 2, lax.axis_index("yl")
    blocks = gain.reshape(TILES // 4, -1, gain.shape[1])
    got = []
    for a, b, n in itertools.product(range(2), repeat=3):
        turn = [
            (((s * 2 + h) * 2 + w) * 2 + y, (((h ^ a) * 2 + s) * 2 + (w ^ b)) * 2 + (y ^ n))
            for s, h, w, y in itertools.product(range(2), repeat=4)
        ]
        block = lax.dynamic_index_in_dim(blocks, (low ^ b) * 2 + (yl ^ n), 0, keepdims=False)
        got.append(lax.ppermute(block, ("core", "x", "yl"), turn))
    return got


def shards(jacobian, gain, variance):
    rows, width = jacobian.shape
    chunks = width // TILES // LANES
    parts = jacobian.reshape(rows, TILES, chunks, LANES).transpose(1, 0, 2, 3)
    parts = parts.reshape(TILES, rows * chunks, LANES)
    far, near = pick(parts)
    far = exchange(far, "z").reshape(TILES, FAR * rows * chunks, LANES)
    near = [near[m].reshape(NEAR * rows * chunks, LANES) for m in range(QUAD)]
    for m in range(1, QUAD):
        near[m] = lax.ppermute(near[m], "z", [(s, s ^ m) for s in range(TILES)])
    columns = retile(gain)
    sent = spread(far, near, rows, chunks)
    xy = exchange(sent, PLANE)
    partial = tile(xy, columns, rows, chunks)
    in_plane = exchange(partial, PLANE).sum(axis=0)
    in_plane = in_plane[: rows * TILES].reshape(rows, TILES).transpose(1, 0)
    return variance - exchange(in_plane, "z").sum(axis=0)


def solution(mesh):
    devices = mesh.devices.reshape(2, 2, TILES, 4, 2)
    return jax.shard_map(
        shards,
        mesh=Mesh(devices, ALL),
        in_specs=(P(ALL, None), P(("yh", "core"), ("z", "x", "yl")), P(ALL)),
        out_specs=P(ALL),
        check_vma=False,
    )
```

```python
import functools
import itertools

import jax
import jax.numpy as jnp
from jax import lax
from jax.experimental import pallas as pl
from jax.experimental.pallas import tpu as pltpu
from jax.sharding import Mesh
from jax.sharding import PartitionSpec as P


PLANE = ("yh", "x", "yl")
ALL = ("yh", "core", "z", "x", "yl")
F32 = jnp.float32
BF16 = jnp.bfloat16
TILES = 16
HALF = TILES // 2
QUAD = 4
FAR = 7
NEAR = 8
LANES = 128
VMEM = pl.BlockSpec(memory_space=pltpu.VMEM)


def plane_index():
    return (lax.axis_index("yh") * 4 + lax.axis_index("x")) * 2 + lax.axis_index("yl")


def half_of(c, z):
    apart = jnp.where(c // QUAD < z // QUAD, 1, 0) ^ (c & 1) ^ (z & 1)
    turn = (z - c) & 3
    beside = jnp.where(turn == 2, 1 ^ ((z >> 1) & 1), turn >> 1)
    return jnp.where(c // QUAD == z // QUAD, beside, apart)


def block_for(z, half, quad, second):
    beside = z ^ 2 if second else (z // QUAD) * QUAD + ((z + 2 * half - 1) & 3)
    apart = QUAD * quad + 2 * second + (half ^ jnp.where(quad < z // QUAD, 1, 0) ^ (z & 1))
    return jnp.where(quad == z // QUAD, beside, apart)


def exchange(parts, axis):
    return lax.all_to_all(parts, axis, split_axis=0, concat_axis=0, tiled=True)


def pick_kernel(in_ref, far_ref, near_ref):
    mine = lax.axis_index("z")
    half = lax.axis_index("yh") ^ (mine & 1)
    for z in range(TILES):
        for slot in range(FAR - 1):
            quad = slot // 2 + jnp.where(slot // 2 >= mine // QUAD, 1, 0)
            far_ref[z, slot] = in_ref[block_for(z, half, quad, slot % 2)]
        far_ref[z, FAR - 1] = in_ref[z]
    for m in range(QUAD):
        z = mine ^ m
        for slot in range(NEAR):
            quad = slot // 2 + jnp.where(slot // 2 >= mine // QUAD, 1, 0)
            if slot < FAR - 1:
                near_ref[m, slot] = in_ref[block_for(z, 1 - half, quad, slot % 2)]
            else:
                near_ref[m, slot] = in_ref[block_for(z, half, mine // QUAD, slot % 2)]


def pick(parts):
    return pl.pallas_call(
        pick_kernel,
        out_shape=(
            jax.ShapeDtypeStruct((TILES, FAR, *parts.shape[1:]), BF16),
            jax.ShapeDtypeStruct((QUAD, NEAR, *parts.shape[1:]), BF16),
        ),
        in_specs=[VMEM],
        out_specs=(VMEM, VMEM),
        cost_estimate=pl.CostEstimate(flops=1_000_000, bytes_accessed=900_000, transcendentals=0),
        compiler_params=pltpu.CompilerParams(vmem_limit_bytes=4 * 1024 * 1024),
        name="pick",
    )(parts)


def spread_kernel(rows, chunks, far_ref, *refs):
    *near_refs, out_ref, wide, stage = refs
    z = lax.axis_index("z")
    top = lax.axis_index("yh")
    block = rows * chunks
    step = FAR * block
    near_at = TILES * step
    for s in range(TILES):
        wide[s * step : (s + 1) * step, :] = far_ref[s].astype(F32)
    for m in range(QUAD):
        at = near_at + m * NEAR * block
        wide[at : at + NEAR * block, :] = near_refs[m][...].astype(F32)

    @pl.loop(0, TILES)
    def _(to):
        diagonal = to == z
        quad = to // QUAD
        beside = quad == z // QUAD
        half_x = jnp.where(diagonal, 0, half_of(to, z))
        half_y = jnp.where(diagonal, 1, half_x)
        second = jnp.where(beside, jnp.where(((z - to) & 3) == 2, 1, 0), (to >> 1) & 1)
        for k in range(HALF):
            swapped = quad == k // 2
            for side, half in ((0, half_x), (1, half_y)):
                parity = half ^ top
                s = 2 * k + parity
                near_s = (z // QUAD) * QUAD + 2 * (k % 2) + jnp.where(beside, parity, 1 - parity)
                last = FAR - 1
                if side == 0:
                    slot = 2 * (quad - jnp.where(quad > k // 2, 1, 0)) + second
                    far = s * FAR + jnp.where(diagonal, last, slot)
                    near_slot = 2 * (quad - jnp.where(quad > z // QUAD, 1, 0)) + second
                    near_slot = jnp.where(beside, last + second, near_slot)
                    near = TILES * FAR + (near_s ^ z) * NEAR + near_slot
                    use_near = jnp.logical_and(swapped, jnp.logical_not(diagonal))
                else:
                    far = s * FAR + last
                    near = near_s * FAR + last
                    use_near = jnp.logical_and(swapped, jnp.logical_not(beside))
                at = pl.multiple_of(jnp.where(use_near, near, far) * block, HALF)
                stage[side, k * block : (k + 1) * block, :] = wide[pl.ds(at, block), :]
        for side in range(2):
            for q in range(chunks):
                got = [
                    stage[side, pl.ds(r * chunks + q, HALF, stride=block), :] for r in range(rows)
                ]
                out_ref[to, side * chunks + q] = jnp.concatenate(got, axis=0).astype(BF16)


def spread(far, near, rows, chunks):
    block = rows * chunks
    return pl.pallas_call(
        functools.partial(spread_kernel, rows, chunks),
        out_shape=jax.ShapeDtypeStruct((TILES, 2 * chunks, HALF * rows, LANES), BF16),
        in_specs=[VMEM] * (1 + len(near)),
        out_specs=VMEM,
        scratch_shapes=[
            pltpu.VMEM(((TILES * FAR + QUAD * NEAR) * block, LANES), F32),
            pltpu.VMEM((2, HALF * block, LANES), F32),
        ],
        cost_estimate=pl.CostEstimate(flops=4_000_000, bytes_accessed=2_500_000, transcendentals=0),
        compiler_params=pltpu.CompilerParams(vmem_limit_bytes=8 * 1024 * 1024),
        name="spread",
    )(far, *near)


def tile_kernel(rows, chunks, xy_ref, own_ref, other_ref, out_ref, narrow, left):
    z = lax.axis_index("z")
    x = lax.axis_index("x")
    yl = lax.axis_index("yl")
    core = lax.axis_index("core")
    c = plane_index()
    group = HALF * rows
    total = TILES * group
    deep = chunks * LANES
    diagonal = c == z
    half_x = jnp.where(diagonal, 0, half_of(c, z))
    half_y = jnp.where(diagonal, 1, half_x)
    beside = c // QUAD == z // QUAD
    for q in range(chunks):
        lane = q * LANES
        for s in range(TILES):
            for kind in range(2):
                start = kind * total + s * group
                got = xy_ref[s, kind * chunks + q]
                left[start : start + group, lane : lane + LANES] = got
                narrow[kind, q, s * group : (s + 1) * group, :] = got
    acc_x = jnp.zeros((total, LANES), F32)
    acc_y = jnp.zeros((total, LANES), F32)
    kind_x = jnp.where(diagonal, 0, 1)
    for m in range(chunks // 2):
        half_ref, at = (own_ref, other_ref)[m // 2], m % 2 * 2 * deep
        columns = jnp.concatenate([half_ref[at : at + deep, :], half_ref[at + deep : at + 2 * deep, :]], axis=1)
        product = jnp.dot(left[...], columns, preferred_element_type=F32)
        for n in range(2):
            k = ((core ^ (m // 2)) * 2 + ((x & 1) ^ (m % 2))) * 2 + (yl ^ n)
            part = product[:, n * LANES : (n + 1) * LANES]
            acc_x += part[:total] * narrow[kind_x, k].astype(F32)
            acc_y += part[total:] * narrow[1, k].astype(F32)
    ones = jnp.ones((LANES, LANES), F32)
    sum_x, sum_y = (
        jnp.dot(acc, ones, precision=lax.Precision.HIGHEST, preferred_element_type=F32)
        for acc in (acc_x, acc_y)
    )
    lane = lax.broadcasted_iota(jnp.int32, (group, LANES), 1)
    row = lax.broadcasted_iota(jnp.int32, (group, LANES), 0)
    r, k = row // HALF, row % HALF
    scale_x = jnp.where(diagonal, 1.0, 2.0)
    for top in range(2):
        parity = half_x ^ top
        swapped = jnp.logical_and(k // 2 == c // QUAD, jnp.logical_not(beside))
        plane = jnp.where(swapped, (z // QUAD) * QUAD + 2 * (k % 2) + 1 - parity, 2 * k + parity)
        mine_x = lane == r * TILES + plane
        mine_y = jnp.logical_and(lane == r * TILES + 2 * k + (half_y ^ top), diagonal)
        for s in range(top * HALF, (top + 1) * HALF):
            got = jnp.where(mine_x, sum_x[s * group : (s + 1) * group] * scale_x, 0.0)
            got = jnp.where(mine_y, sum_y[s * group : (s + 1) * group], got)
            out_ref[s : s + 1, :] = jnp.sum(got, axis=0, keepdims=True)


def tile(xy, own, other, rows, chunks):
    total = TILES * HALF * rows
    flops = 2 * 2 * total * (chunks * LANES) ** 2
    return pl.pallas_call(
        functools.partial(tile_kernel, rows, chunks),
        out_shape=jax.ShapeDtypeStruct((TILES, LANES), F32),
        in_specs=[VMEM] * 3,
        out_specs=VMEM,
        scratch_shapes=[
            pltpu.VMEM((2, chunks, total, LANES), BF16),
            pltpu.VMEM((2 * total, chunks * LANES), BF16),
        ],
        cost_estimate=pl.CostEstimate(flops=flops, bytes_accessed=4_000_000, transcendentals=0),
        compiler_params=pltpu.CompilerParams(vmem_limit_bytes=16 * 1024 * 1024),
        name="tile",
    )(xy, own, other)


def retile(gain):
    low, yl = lax.axis_index("x") % 2, lax.axis_index("yl")
    blocks = gain.reshape(TILES // 4, -1, gain.shape[1])
    got = []
    for b, n in itertools.product(range(2), repeat=2):
        turn = [
            (((s * 2 + h) * 2 + w) * 2 + y, ((h * 2 + s) * 2 + (w ^ b)) * 2 + (y ^ n))
            for s, h, w, y in itertools.product(range(2), repeat=4)
        ]
        block = lax.dynamic_index_in_dim(blocks, (low ^ b) * 2 + (yl ^ n), 0, keepdims=False)
        got.append(lax.ppermute(block, ("core", "x", "yl"), turn))
    return jnp.concatenate(got, axis=0)


def shards(jacobian, gain, variance):
    rows, width = jacobian.shape
    chunks = width // TILES // LANES
    parts = jacobian.reshape(rows, TILES, chunks, LANES).transpose(1, 0, 2, 3)
    parts = parts.reshape(TILES, rows * chunks, LANES)
    far, near = pick(parts)
    far = exchange(far, "z").reshape(TILES, FAR * rows * chunks, LANES)
    near = [near[m].reshape(NEAR * rows * chunks, LANES) for m in range(QUAD)]
    for m in range(1, QUAD):
        near[m] = lax.ppermute(near[m], "z", [(s, s ^ m) for s in range(TILES)])
    own = retile(gain)
    other = lax.ppermute(own, "core", [(0, 1), (1, 0)])
    sent = spread(far, near, rows, chunks)
    xy = exchange(sent, PLANE)
    partial = tile(xy, own, other, rows, chunks)
    in_plane = exchange(partial, PLANE).sum(axis=0)
    in_plane = in_plane[: rows * TILES].reshape(rows, TILES).transpose(1, 0)
    return variance - exchange(in_plane, "z").sum(axis=0)


def solution(mesh):
    devices = mesh.devices.reshape(2, 2, TILES, 4, 2)
    return jax.shard_map(
        shards,
        mesh=Mesh(devices, ALL),
        in_specs=(P(ALL, None), P(("yh", "core"), ("z", "x", "yl")), P(ALL)),
        out_specs=P(ALL),
        check_vma=False,
    )
```

```python
import functools
import itertools

import jax
import jax.numpy as jnp
from jax import lax
from jax.experimental import pallas as pl
from jax.experimental.pallas import tpu as pltpu
from jax.sharding import Mesh
from jax.sharding import PartitionSpec as P


PLANE = ("yh", "x", "yl")
ALL = ("yh", "core", "z", "x", "yl")
F32 = jnp.float32
BF16 = jnp.bfloat16
TILES = 16
HALF = TILES // 2
QUAD = 4
FAR = 7
NEAR = 8
LANES = 128
VMEM = pl.BlockSpec(memory_space=pltpu.VMEM)


def plane_index():
    return (lax.axis_index("yh") * 4 + lax.axis_index("x")) * 2 + lax.axis_index("yl")


def half_of(c, z):
    apart = jnp.where(c // QUAD < z // QUAD, 1, 0) ^ (c & 1) ^ (z & 1)
    turn = (z - c) & 3
    beside = jnp.where(turn == 2, 1 ^ ((z >> 1) & 1), turn >> 1)
    return jnp.where(c // QUAD == z // QUAD, beside, apart)


def block_for(z, half, quad, second):
    beside = z ^ 2 if second else (z // QUAD) * QUAD + ((z + 2 * half - 1) & 3)
    apart = QUAD * quad + 2 * second + (half ^ jnp.where(quad < z // QUAD, 1, 0) ^ (z & 1))
    return jnp.where(quad == z // QUAD, beside, apart)


def exchange(parts, axis):
    return lax.all_to_all(parts, axis, split_axis=0, concat_axis=0, tiled=True)


def pick_kernel(in_ref, far_ref, near_ref):
    mine = lax.axis_index("z")
    half = lax.axis_index("yh") ^ (mine & 1)
    for z in range(TILES):
        for slot in range(FAR - 1):
            quad = slot // 2 + jnp.where(slot // 2 >= mine // QUAD, 1, 0)
            far_ref[z, slot] = in_ref[block_for(z, half, quad, slot % 2)]
        far_ref[z, FAR - 1] = in_ref[z]
    for m in range(QUAD):
        z = mine ^ m
        for slot in range(NEAR):
            quad = slot // 2 + jnp.where(slot // 2 >= mine // QUAD, 1, 0)
            if slot < FAR - 1:
                near_ref[m, slot] = in_ref[block_for(z, 1 - half, quad, slot % 2)]
            else:
                near_ref[m, slot] = in_ref[block_for(z, half, mine // QUAD, slot % 2)]


def pick(parts):
    return pl.pallas_call(
        pick_kernel,
        out_shape=(
            jax.ShapeDtypeStruct((TILES, FAR, *parts.shape[1:]), BF16),
            jax.ShapeDtypeStruct((QUAD, NEAR, *parts.shape[1:]), BF16),
        ),
        in_specs=[VMEM],
        out_specs=(VMEM, VMEM),
        cost_estimate=pl.CostEstimate(flops=1_000_000, bytes_accessed=900_000, transcendentals=0),
        compiler_params=pltpu.CompilerParams(vmem_limit_bytes=4 * 1024 * 1024),
        name="pick",
    )(parts)


def spread_kernel(rows, chunks, far_ref, *refs):
    *near_refs, out_ref, wide, stage = refs
    z = lax.axis_index("z")
    top = lax.axis_index("yh")
    block = rows * chunks
    step = FAR * block
    near_at = TILES * step
    for s in range(TILES):
        wide[s * step : (s + 1) * step, :] = far_ref[s].astype(F32)
    for m in range(QUAD):
        at = near_at + m * NEAR * block
        wide[at : at + NEAR * block, :] = near_refs[m][...].astype(F32)

    @pl.loop(0, TILES, unroll=4)
    def _(to):
        diagonal = to == z
        quad = to // QUAD
        beside = quad == z // QUAD
        half_x = jnp.where(diagonal, 0, half_of(to, z))
        half_y = jnp.where(diagonal, 1, half_x)
        second = jnp.where(beside, jnp.where(((z - to) & 3) == 2, 1, 0), (to >> 1) & 1)
        for k in range(HALF):
            swapped = quad == k // 2
            for side, half in ((0, half_x), (1, half_y)):
                parity = half ^ top
                s = 2 * k + parity
                near_s = (z // QUAD) * QUAD + 2 * (k % 2) + jnp.where(beside, parity, 1 - parity)
                last = FAR - 1
                if side == 0:
                    slot = 2 * (quad - jnp.where(quad > k // 2, 1, 0)) + second
                    far = s * FAR + jnp.where(diagonal, last, slot)
                    near_slot = 2 * (quad - jnp.where(quad > z // QUAD, 1, 0)) + second
                    near_slot = jnp.where(beside, last + second, near_slot)
                    near = TILES * FAR + (near_s ^ z) * NEAR + near_slot
                    use_near = jnp.logical_and(swapped, jnp.logical_not(diagonal))
                else:
                    far = s * FAR + last
                    near = near_s * FAR + last
                    use_near = jnp.logical_and(swapped, jnp.logical_not(beside))
                at = pl.multiple_of(jnp.where(use_near, near, far) * block, HALF)
                stage[side, k * block : (k + 1) * block, :] = wide[pl.ds(at, block), :]
        for side in range(2):
            for q in range(chunks):
                got = [
                    stage[side, pl.ds(r * chunks + q, HALF, stride=block), :] for r in range(rows)
                ]
                out_ref[to, side * chunks + q] = jnp.concatenate(got, axis=0).astype(BF16)


def spread(far, near, rows, chunks):
    block = rows * chunks
    return pl.pallas_call(
        functools.partial(spread_kernel, rows, chunks),
        out_shape=jax.ShapeDtypeStruct((TILES, 2 * chunks, HALF * rows, LANES), BF16),
        in_specs=[VMEM] * (1 + len(near)),
        out_specs=VMEM,
        scratch_shapes=[
            pltpu.VMEM(((TILES * FAR + QUAD * NEAR) * block, LANES), F32),
            pltpu.VMEM((2, HALF * block, LANES), F32),
        ],
        cost_estimate=pl.CostEstimate(flops=4_000_000, bytes_accessed=2_500_000, transcendentals=0),
        compiler_params=pltpu.CompilerParams(vmem_limit_bytes=8 * 1024 * 1024),
        name="spread",
    )(far, *near)


def tile_kernel(rows, chunks, xy_ref, own_ref, other_ref, out_ref, left):
    z = lax.axis_index("z")
    x = lax.axis_index("x")
    yl = lax.axis_index("yl")
    core = lax.axis_index("core")
    c = plane_index()
    group = HALF * rows
    total = TILES * group
    deep = chunks * LANES
    diagonal = c == z
    half_x = jnp.where(diagonal, 0, half_of(c, z))
    half_y = jnp.where(diagonal, 1, half_x)
    beside = c // QUAD == z // QUAD
    for q in range(chunks):
        lane = q * LANES
        for s in range(TILES):
            for kind in range(2):
                start = kind * total + s * group
                got = xy_ref[s, kind * chunks + q]
                left[start : start + group, lane : lane + LANES] = got
    acc_x = jnp.zeros((total, LANES), F32)
    acc_y = jnp.zeros((total, LANES), F32)
    top_x = pl.multiple_of(jnp.where(diagonal, 0, total), HALF)
    for m in range(chunks // 2):
        half_ref, at = (own_ref, other_ref)[m // 2], m % 2 * 2 * deep
        columns = jnp.concatenate([half_ref[at : at + deep, :], half_ref[at + deep : at + 2 * deep, :]], axis=1)
        product = jnp.dot(left[...], columns, preferred_element_type=F32)
        for n in range(2):
            k = ((core ^ (m // 2)) * 2 + ((x & 1) ^ (m % 2))) * 2 + (yl ^ n)
            part = product[:, n * LANES : (n + 1) * LANES]
            lanes = pl.ds(pl.multiple_of(k * LANES, LANES), LANES)
            acc_x += part[:total] * left[pl.ds(top_x, total), lanes].astype(F32)
            acc_y += part[total:] * left[total:, lanes].astype(F32)
    sum_x, sum_y = (jnp.sum(acc, axis=1, keepdims=True) for acc in (acc_x, acc_y))
    lane = lax.broadcasted_iota(jnp.int32, (group, LANES), 1)
    row = lax.broadcasted_iota(jnp.int32, (group, LANES), 0)
    r, k = row // HALF, row % HALF
    scale_x = jnp.where(diagonal, 1.0, 2.0)
    for top in range(2):
        parity = half_x ^ top
        swapped = jnp.logical_and(k // 2 == c // QUAD, jnp.logical_not(beside))
        plane = jnp.where(swapped, (z // QUAD) * QUAD + 2 * (k % 2) + 1 - parity, 2 * k + parity)
        mine_x = lane == r * TILES + plane
        mine_y = jnp.logical_and(lane == r * TILES + 2 * k + (half_y ^ top), diagonal)
        for s in range(top * HALF, (top + 1) * HALF):
            got = jnp.where(mine_x, sum_x[s * group : (s + 1) * group] * scale_x, 0.0)
            got = jnp.where(mine_y, sum_y[s * group : (s + 1) * group], got)
            out_ref[s : s + 1, :] = jnp.sum(got, axis=0, keepdims=True)


def tile(xy, own, other, rows, chunks):
    total = TILES * HALF * rows
    flops = 2 * 2 * total * (chunks * LANES) ** 2
    return pl.pallas_call(
        functools.partial(tile_kernel, rows, chunks),
        out_shape=jax.ShapeDtypeStruct((TILES, LANES), F32),
        in_specs=[VMEM] * 3,
        out_specs=VMEM,
        scratch_shapes=[
            pltpu.VMEM((2 * total, chunks * LANES), BF16),
        ],
        cost_estimate=pl.CostEstimate(flops=flops, bytes_accessed=4_000_000, transcendentals=0),
        compiler_params=pltpu.CompilerParams(vmem_limit_bytes=16 * 1024 * 1024),
        name="tile",
    )(xy, own, other)


def retile(gain):
    low, yl = lax.axis_index("x") % 2, lax.axis_index("yl")
    blocks = gain.reshape(TILES // 4, -1, gain.shape[1])
    got = []
    for b, n in itertools.product(range(2), repeat=2):
        turn = [
            (((s * 2 + h) * 2 + w) * 2 + y, ((h * 2 + s) * 2 + (w ^ b)) * 2 + (y ^ n))
            for s, h, w, y in itertools.product(range(2), repeat=4)
        ]
        block = lax.dynamic_index_in_dim(blocks, (low ^ b) * 2 + (yl ^ n), 0, keepdims=False)
        got.append(lax.ppermute(block, ("core", "x", "yl"), turn))
    return jnp.concatenate(got, axis=0)


def shards(jacobian, gain, variance):
    rows, width = jacobian.shape
    chunks = width // TILES // LANES
    parts = jacobian.reshape(rows, TILES, chunks, LANES).transpose(1, 0, 2, 3)
    parts = parts.reshape(TILES, rows * chunks, LANES)
    far, near = pick(parts)
    far = exchange(far, "z").reshape(TILES, FAR * rows * chunks, LANES)
    near = [near[m].reshape(NEAR * rows * chunks, LANES) for m in range(QUAD)]
    for m in range(1, QUAD):
        near[m] = lax.ppermute(near[m], "z", [(s, s ^ m) for s in range(TILES)])
    own = retile(gain)
    other = lax.ppermute(own, "core", [(0, 1), (1, 0)])
    sent = spread(far, near, rows, chunks)
    xy = exchange(sent, PLANE)
    partial = tile(xy, own, other, rows, chunks)
    in_plane = exchange(partial, PLANE).sum(axis=0)
    in_plane = in_plane[: rows * TILES].reshape(rows, TILES).transpose(1, 0)
    return variance - exchange(in_plane, "z").sum(axis=0)


def solution(mesh):
    devices = mesh.devices.reshape(2, 2, TILES, 4, 2)
    return jax.shard_map(
        shards,
        mesh=Mesh(devices, ALL),
        in_specs=(P(ALL, None), P(("yh", "core"), ("z", "x", "yl")), P(ALL)),
        out_specs=P(ALL),
        check_vma=False,
    )
```
